32 devices in a mesh: seq: 8 (over z, core), mp: 4 (over y, x).
Axes of the slice: x: 2, y: 2, z: 4, core: 2. Of those that a mesh axis runs over, the one named last changes fastest.
Arguments:
- hidden_in: bfloat16 [4096, 4096], P('seq', 'mp'), may hold values from -30 to 30
- norm_gain: float32 [4096], replicated, may hold values from 0.1 to 1.9
- w_z: bfloat16 [4096, 8192], P('seq', 'mp'), may hold values from -0.09375 to 0.09375
- w_x: bfloat16 [4096, 8192], P('seq', 'mp'), may hold values from -0.09375 to 0.09375
- w_b: bfloat16 [4096, 1024], P('seq', 'mp'), may hold values from -0.09375 to 0.09375
- w_c: bfloat16 [4096, 1024], P('seq', 'mp'), may hold values from -0.09375 to 0.09375
- w_dt: bfloat16 [4096, 128], P('seq', 'mp'), may hold values from -0.0625 to 0.0625
- conv_x: float32 [4, 8192], P(None, 'mp'), may hold values from -3 to 3
- conv_b: float32 [4, 1024], P(None, 'mp'), may hold values from -3 to 3
- conv_c: float32 [4, 1024], P(None, 'mp'), may hold values from -3 to 3
- dt_bias: float32 [128], P('mp'), may hold values from -9 to -5
- a_rate: float32 [128], P('mp'), may hold values from 0.5 to 16
- skip_gain: float32 [128], P('mp'), may hold values from -3 to 3
- group_gain: float32 [8192], P('mp'), may hold values from 0.1 to 1.9
- w_out: bfloat16 [8192, 4096], P('mp', 'seq'), may hold values from -0.0625 to 0.0625
- attn_gain: float32 [4096], replicated, may hold values from 0.1 to 1.9
- w_q: bfloat16 [4096, 4096], P(None, 'mp'), may hold values from -0.125 to 0.125
- w_k: bfloat16 [4096, 1024], P(None, 'mp'), may hold values from -0.125 to 0.125
- w_v: bfloat16 [4096, 1024], P(None, 'mp'), may hold values from -0.09375 to 0.09375
Outputs:
- mixed: float32 [4096, 4096], P('seq', 'mp')
- context: float32 [4096, 4096], P('seq', 'mp')
The draws below stay inside these ranges and needn't reach their ends.
All inputs are finite; a program needn't handle non-finite values.
Results may differ from the reference program's by a relative error of at most 0.017.
Values may be sent and summed in bfloat16 or wider, within the bound.
No kernel may reach another device: no remote copies, remote signals or barrier semaphores. Data moves between devices by JAX's collectives and lax.ppermute only.
A program may use at most 192 MiB of HBM per device.

```python
import math
import jax
import jax.numpy as jnp
from jax import lax

D = 4096
DI = 8192
H = 128
P_SIZE = 64
N = 128
G = 8
KW = 4
HQ = 32
HK = 8
HD = 128
WINDOW = 4096
QB = 128
TOK_DEV = 512
TOKENS = 4096
N_SEQ = 8
N_MP = 4


def contiguous_spans(key):
    forward_sense = jnp.clip(jax.random.normal(jax.random.fold_in(key, 101), (D,), jnp.float32), -4.0, 4.0)
    processor_slots = jax.random.randint(jax.random.fold_in(key, 102), (TOKENS // TOK_DEV * 2,), 0, TOKENS)
    input_magnitude = jax.random.uniform(jax.random.fold_in(key, 103), (TOKENS // TOK_DEV * 2,), jnp.float32, 0.6, 1.0)
    return (forward_sense, processor_slots, input_magnitude)


def draw_hidden_in(key, part):
    forward_sense, processor_slots, input_magnitude = contiguous_spans(key)
    base = jnp.clip(jax.random.normal(jax.random.fold_in(key, 1), (TOKENS, D), jnp.float32), -6.0, 6.0)
    mixing = jnp.zeros((TOKENS,), jnp.float32).at[processor_slots].set(input_magnitude)
    values = base * (1.0 - mixing)[:, None] + forward_sense[None, :] * (4.0 * mixing)[:, None]
    return jnp.clip(values, -30.0, 30.0).astype(jnp.bfloat16)


def draw_w_dt(key, part):
    forward_sense, processor_slots, input_magnitude = contiguous_spans(key)
    noise = 0.3 * jnp.clip(jax.random.normal(jax.random.fold_in(key, 3), (D, H), jnp.float32), -6.0, 6.0) / math.sqrt(D)
    lifted = jax.random.uniform(jax.random.fold_in(key, 4), (H,), jnp.float32, 6.0, 10.0)
    limit = 4.0 / math.sqrt(D)
    return jnp.clip(noise + forward_sense[:, None] * lifted[None, :] / D, -limit, limit).astype(jnp.bfloat16)


def draw_w_q(key, part):
    base = jnp.clip(jax.random.normal(jax.random.fold_in(key, 5), (D, HQ * HD), jnp.float32), -6.0, 6.0) / math.sqrt(D)
    limit = 8.0 / math.sqrt(D)
    return jnp.clip(base, -limit, limit).astype(jnp.bfloat16)


def draw_w_k(key, part):
    base = jnp.clip(jax.random.normal(jax.random.fold_in(key, 6), (D, HK * HD), jnp.float32), -6.0, 6.0) / math.sqrt(D)
    limit = 8.0 / math.sqrt(D)
    return jnp.clip(base, -limit, limit).astype(jnp.bfloat16)


def block_levels(own_key, dims, split, smallest, largest):
    factor_of, own = 1.0, jax.random.fold_in(own_key, 6)
    for position, blocks in split:
        draws = jnp.exp(jax.random.uniform(jax.random.fold_in(own, position), (blocks,), jnp.float32, smallest / len(split), largest / len(split)))
        factor_of = factor_of * jnp.repeat(draws, dims[position] // blocks).reshape([-1 if axis == position else 1 for axis in range(len(dims))])
    return factor_of


def scatter_about(own_key, dims, scale, bound, split=(), kind=jnp.bfloat16):
    result = scale * jax.random.normal(own_key, dims, jnp.float32)
    if split:
        result = result * block_levels(own_key, dims, split, -0.22, 0.18)
    return jnp.clip(result, -bound, bound).astype(kind)


def setup_inputs(seed: int = 0) -> dict:
    key_list = jax.random.split(jax.random.key(seed), 20)
    return {
        "hidden_in": draw_hidden_in(jax.random.fold_in(key_list[19], 71), 0),
        "norm_gain": jnp.clip(1.0 + 0.18 * jax.random.normal(key_list[1], (D,), jnp.float32), 0.1, 1.9),
        "w_z": scatter_about(key_list[2], (D, DI), D ** -0.5, 0.09375, ((0, 8), (1, 4))),
        "w_x": scatter_about(key_list[3], (D, DI), D ** -0.5, 0.09375, ((0, 8), (1, 4))),
        "w_b": scatter_about(key_list[4], (D, G * N), D ** -0.5, 0.09375, ((0, 8), (1, 4))),
        "w_c": scatter_about(key_list[5], (D, G * N), D ** -0.5, 0.09375, ((0, 8), (1, 4))),
        "w_dt": draw_w_dt(jax.random.fold_in(key_list[19], 71), 0),
        "conv_x": scatter_about(key_list[7], (KW, DI), 0.5, 3.0, ((1, 4),), jnp.float32),
        "conv_b": scatter_about(key_list[8], (KW, G * N), 0.5, 3.0, ((1, 4),), jnp.float32),
        "conv_c": scatter_about(key_list[9], (KW, G * N), 0.5, 3.0, ((1, 4),), jnp.float32),
        "dt_bias": jnp.clip(-9.0 + 4.0 * jax.random.uniform(key_list[10], (H,), jnp.float32) ** block_levels(key_list[10], (H,), ((0, 4),), -0.2, 0.2), -9.0, -5.0),
        "a_rate": jnp.clip(jnp.exp(math.log(16.0) - 3.465736 * jax.random.uniform(key_list[11], (H,), jnp.float32) ** block_levels(key_list[11], (H,), ((0, 4),), -0.2, 0.2)), 0.5, 16.0),
        "skip_gain": scatter_about(key_list[12], (H,), 1.0, 3.0, ((0, 4),), jnp.float32),
        "group_gain": jnp.clip(1.0 + 0.18 * jax.random.normal(key_list[13], (DI,), jnp.float32), 0.1, 1.9),
        "w_out": scatter_about(key_list[14], (DI, D), DI ** -0.5, 0.0625, ((0, 4), (1, 8))),
        "attn_gain": jnp.clip(1.0 + 0.18 * jax.random.normal(key_list[15], (D,), jnp.float32), 0.1, 1.9),
        "w_q": draw_w_q(jax.random.fold_in(key_list[19], 71), 0),
        "w_k": draw_w_k(jax.random.fold_in(key_list[19], 71), 0),
        "w_v": scatter_about(key_list[18], (D, HK * HD), D ** -0.5, 0.09375, ((1, 4),)),
    }


HIGH = lax.Precision.HIGHEST

def rms_norm(values, gain):
    return values * lax.rsqrt(lax.optimization_barrier(jnp.mean(values * values, axis=-1, keepdims=True)) + 1e-05) * gain

def causal_conv(values, rim, device_routine):
    padded = jnp.concatenate([rim, values], axis=0)
    length = values.shape[0]
    summed = jnp.zeros(values.shape, jnp.float32)
    for offset in range(device_routine.shape[0]):
        summed = summed + device_routine[offset][None, :] * padded[offset:offset + length]
    return jax.nn.silu(summed)

def ssd_block(carry_state, pieces):
    inputs, step_sizes, decays, keys_b, reads_c = pieces
    per_group = inputs.shape[1] // keys_b.shape[1]
    b_heads = jnp.repeat(keys_b, per_group, axis=1)
    c_heads = jnp.repeat(reads_c, per_group, axis=1)
    cumulative = jnp.cumsum(decays, axis=0)
    length = inputs.shape[0]
    causal_mask = jnp.arange(length)[:, None] >= jnp.arange(length)[None, :]
    spread = cumulative[:, None, :] - cumulative[None, :, :]
    within = jnp.exp(jnp.where(causal_mask[:, :, None], spread, -jnp.inf))
    affinity = jnp.einsum('tgn,sgn->gts', reads_c, keys_b, precision=HIGH)
    affinity = jnp.repeat(affinity, per_group, axis=0)
    mixing = affinity * jnp.transpose(within, (2, 0, 1)) * jnp.transpose(step_sizes)[:, None, :]
    inside = jnp.einsum('hts,shp->thp', mixing, inputs, precision=HIGH)
    carried = jnp.exp(cumulative)[:, :, None] * jnp.einsum('thn,hpn->thp', c_heads, carry_state, precision=HIGH)
    tail_weight = jnp.exp(cumulative[-1][None, :] - cumulative) * step_sizes
    fresh_state = jnp.einsum('sh,shp,shn->hpn', tail_weight, inputs, b_heads, precision=HIGH)
    updated = jnp.exp(cumulative[-1])[:, None, None] * carry_state + fresh_state
    return (updated, inside + carried)

def run_ssd(inputs, step_sizes, decays, keys_b, reads_c, block, carry_state):
    total_rows = inputs.shape[0]
    block_count = total_rows // block

    def blocked(values):
        return values.reshape((block_count, block) + values.shape[1:])
    final_state, outputs = lax.scan(ssd_block, carry_state, (blocked(inputs), blocked(step_sizes), blocked(decays), blocked(keys_b), blocked(reads_c)))
    return (final_state, outputs.reshape((total_rows,) + outputs.shape[2:]))

def window_attention(asking_vectors, keys, values, shift_rows, first_key):
    per_kv = asking_vectors.shape[1] // keys.shape[1]
    keys_all = jnp.repeat(keys, per_kv, axis=1)
    values_all = jnp.repeat(values, per_kv, axis=1)
    query_rows = asking_vectors.shape[0]
    key_count = keys.shape[0]
    scale = asking_vectors.shape[2] ** (-0.5)
    index_offsets = jnp.arange(key_count)[None, :] - shift_rows - jnp.arange(query_rows)[:, None]
    allowed = (index_offsets <= 0) & (index_offsets > -WINDOW) & (first_key + jnp.arange(key_count) >= 0)[None, :]

    def one_head(operands):
        query_h, key_h, value_h = operands
        scores = lax.dot_general(query_h, key_h, (((1,), (1,)), ((), ())), preferred_element_type=jnp.float32) * scale
        scores = jnp.where(allowed, scores, -jnp.inf)
        row_peak = lax.optimization_barrier(jnp.max(scores, axis=1, keepdims=True))
        exp_scores = jnp.exp(scores - row_peak)
        weights = (exp_scores / lax.optimization_barrier(jnp.sum(exp_scores, axis=1, keepdims=True))).astype(jnp.bfloat16)
        return jnp.dot(weights, value_h, preferred_element_type=jnp.float32)
    outputs = lax.map(one_head, (jnp.transpose(asking_vectors, (1, 0, 2)), jnp.transpose(keys_all, (1, 0, 2)), jnp.transpose(values_all, (1, 0, 2))))
    return jnp.transpose(outputs, (1, 0, 2)).reshape(query_rows, -1)

def reference(hidden_in, norm_gain, w_z, w_x, w_b, w_c, w_dt, conv_x, conv_b, conv_c, dt_bias, a_rate, skip_gain, group_gain, w_out, attn_gain, w_q, w_k, w_v):
    stream = hidden_in.astype(jnp.float32)
    normed = rms_norm(stream, norm_gain).astype(jnp.bfloat16)
    gate_proj = jnp.dot(normed, w_z, preferred_element_type=jnp.float32)
    input_mapped = jnp.dot(normed, w_x, preferred_element_type=jnp.float32)
    b_proj = jnp.dot(normed, w_b, preferred_element_type=jnp.float32)
    c_proj = jnp.dot(normed, w_c, preferred_element_type=jnp.float32)
    delta_time_unscaled = jnp.dot(normed, w_dt, preferred_element_type=jnp.float32)
    conv_in = causal_conv(input_mapped, jnp.zeros((KW - 1, DI), jnp.float32), conv_x)
    conv_bv = causal_conv(b_proj, jnp.zeros((KW - 1, G * N), jnp.float32), conv_b)
    conv_cv = causal_conv(c_proj, jnp.zeros((KW - 1, G * N), jnp.float32), conv_c)
    step_sizes = jax.nn.softplus(delta_time_unscaled + dt_bias[None, :])
    decays = -a_rate[None, :] * step_sizes
    inputs = conv_in.reshape(TOKENS, H, P_SIZE)
    final_state, ssd_out = run_ssd(inputs, step_sizes, decays, conv_bv.reshape(TOKENS, G, N), conv_cv.reshape(TOKENS, G, N), QB, jnp.zeros((H, P_SIZE, N), jnp.float32))
    full = ssd_out + skip_gain[None, :, None] * inputs
    gated = full.reshape(TOKENS, DI) * jax.nn.silu(gate_proj)
    grouped = gated.reshape(TOKENS, G, DI // G)
    y_normed = rms_norm(grouped, group_gain.reshape(G, DI // G)).reshape(TOKENS, DI).astype(jnp.bfloat16)
    width = DI // N_MP
    summed = jnp.zeros((TOKENS, D), jnp.float32)
    for member in range(N_MP):
        term = jnp.dot(y_normed[:, member * width:(member + 1) * width], w_out[member * width:(member + 1) * width], preferred_element_type=jnp.float32)
        summed = summed + lax.optimization_barrier(term.astype(jnp.bfloat16)).astype(jnp.float32)
    mixed = stream + summed
    mixed_low = lax.optimization_barrier(mixed.astype(jnp.bfloat16)).astype(jnp.float32)
    normed_two = rms_norm(mixed_low, attn_gain).astype(jnp.bfloat16)
    asking_vectors = jnp.dot(normed_two, w_q, preferred_element_type=jnp.float32).astype(jnp.bfloat16).reshape(TOKENS, HQ, HD)
    keys = jnp.dot(normed_two, w_k, preferred_element_type=jnp.float32).astype(jnp.bfloat16).reshape(TOKENS, HK, HD)
    values = jnp.dot(normed_two, w_v, preferred_element_type=jnp.float32).astype(jnp.bfloat16).reshape(TOKENS, HK, HD)
    keys_pad = jnp.concatenate([jnp.zeros((WINDOW, HK, HD), jnp.bfloat16), keys], axis=0)
    values_pad = jnp.concatenate([jnp.zeros((WINDOW, HK, HD), jnp.bfloat16), values], axis=0)

    def one_block(block_index):
        start = (block_index * TOK_DEV).astype(jnp.int32)
        asking_tile = lax.dynamic_slice_in_dim(asking_vectors, start, TOK_DEV, 0)
        key_blk = lax.dynamic_slice_in_dim(keys_pad, start, WINDOW + TOK_DEV, 0)
        value_blk = lax.dynamic_slice_in_dim(values_pad, start, WINDOW + TOK_DEV, 0)
        return window_attention(asking_tile, key_blk, value_blk, WINDOW, start - WINDOW)
    blocks = lax.map(one_block, jnp.arange(N_SEQ, dtype=jnp.int32))
    context = blocks.reshape(TOKENS, HQ * HD)
    return (mixed, context)
```

```python
import functools

import jax
import jax.numpy as jnp
from jax import lax
from jax.experimental import pallas as pl
from jax.experimental.pallas import tpu as pltpu
from jax.sharding import PartitionSpec as P

P_SIZE = 64
N = 128
HD = 128
WINDOW = 4096
QB = 128
HIGH = lax.Precision.HIGHEST
LOW = jnp.bfloat16
F32 = jnp.float32
MASKED = -1e30


def rms_norm(values, gain):
    return values * lax.rsqrt(jnp.mean(values * values, axis=-1, keepdims=True) + 1e-05) * gain


def swap_cores(block):
    count = lax.axis_size("seq")
    return lax.ppermute(block, "seq", [(i, i ^ 1) for i in range(count)])


def same_core_groups():
    count = lax.axis_size("seq")
    return [list(range(core, count, 2)) for core in range(2)]


def gather_chips(block, axis):
    return lax.all_gather(
        block, "seq", axis=axis, tiled=True, axis_index_groups=same_core_groups()
    )


def in_core_order(core, mine, theirs, axis):
    first = jnp.where(core == 0, mine, theirs)
    second = jnp.where(core == 0, theirs, mine)
    return jnp.concatenate([first, second], axis=axis)


def gather_features(block):
    count = lax.axis_size("mp")
    here = lax.axis_index("mp")
    width = block.shape[1]
    whole = jnp.zeros((block.shape[0], width * count), block.dtype)
    whole = lax.dynamic_update_slice_in_dim(whole, block, here * width, 1)
    for other in range(1, count):
        came = lax.ppermute(block, "mp", [(i, i ^ other) for i in range(count)])
        whole = lax.dynamic_update_slice_in_dim(whole, came, (here ^ other) * width, 1)
    return whole


def scatter_features(block):
    count = lax.axis_size("mp")
    here = lax.axis_index("mp")
    width = block.shape[1] // count
    total = lax.dynamic_slice_in_dim(block, here * width, width, 1).astype(F32)
    for other in range(1, count):
        piece = lax.dynamic_slice_in_dim(block, (here ^ other) * width, width, 1)
        total = total + lax.ppermute(piece, "mp", [(i, i ^ other) for i in range(count)]).astype(F32)
    return total


def dot_nt(a, b):
    return lax.dot_general(a, b, (((1,), (1,)), ((), ())), preferred_element_type=F32)


def dot_tn(a, b):
    return lax.dot_general(a, b, (((0,), (0,)), ((), ())), preferred_element_type=F32)


def head_spread(heads):
    lane = lax.broadcasted_iota(jnp.int32, (heads, heads * P_SIZE), 1) // P_SIZE
    row = lax.broadcasted_iota(jnp.int32, (heads, heads * P_SIZE), 0)
    return (lane == row).astype(F32)


def scan_kernel(x_ref, b_ref, c_ref, step_ref, step_t_ref, rate_ref, rate_t_ref,
                y_ref, grown_ref, state_ref, total_ref, state, total):
    heads = step_ref.shape[1]
    turn = pl.program_id(0)

    @pl.when(turn == 0)
    def _():
        state[...] = jnp.zeros_like(state)
        total[...] = jnp.zeros_like(total)

    row = lax.broadcasted_iota(jnp.int32, (QB, QB), 0)
    col = lax.broadcasted_iota(jnp.int32, (QB, QB), 1)
    causal = row >= col
    lower = causal.astype(F32)
    step = step_ref[...]
    step_t = step_t_ref[...]
    spread_heads = head_spread(heads)
    decay = -rate_ref[...] * step
    decay_t = -rate_t_ref[...] * step_t
    cum = jnp.dot(lower, decay, precision=HIGH, preferred_element_type=F32)
    cum_t = lax.dot_general(decay_t, lower, (((1,), (1,)), ((), ())), precision=HIGH,
                            preferred_element_type=F32)
    last = cum[QB - 1 : QB, :]
    grown_ref[...] = cum + total[...]
    total[...] = total[...] + last
    weights = jnp.concatenate([jnp.exp(cum), jnp.exp(last - cum) * step], axis=0)
    wide = jnp.dot(weights, spread_heads, precision=HIGH, preferred_element_type=F32)
    grow_wide = wide[:QB]
    tail_wide = wide[QB:]
    x = x_ref[...]
    b = b_ref[...]
    c = c_ref[...]
    affinity = dot_nt(c, b)
    before = state[...]
    carried = grow_wide * jnp.dot(c, before.astype(LOW), preferred_element_type=F32)
    fresh = dot_tn(b, (x.astype(F32) * tail_wide).astype(LOW))
    state[...] = grow_wide[QB - 1 : QB, :] * before + fresh
    for pair in range(heads // 2):
        inside = []
        for h in (2 * pair, 2 * pair + 1):
            gap = jnp.where(causal, cum[:, h : h + 1] - cum_t[h : h + 1, :], MASKED)
            mixing = (affinity * jnp.exp(gap) * step_t[h : h + 1, :]).astype(LOW)
            inside.append(
                jnp.dot(mixing, x[:, h * P_SIZE : (h + 1) * P_SIZE], preferred_element_type=F32)
            )
        lanes = slice(2 * pair * P_SIZE, 2 * (pair + 1) * P_SIZE)
        y_ref[:, lanes] = jnp.concatenate(inside, axis=1) + carried[:, lanes]

    @pl.when(turn == pl.num_programs(0) - 1)
    def _():
        state_ref[...] = state[...].astype(LOW)
        total_ref[...] = jnp.dot(jnp.exp(total[...]), spread_heads, precision=HIGH,
                                 preferred_element_type=F32)


def run_scan(x, b, c, step, rate):
    rows, width = x.shape
    heads = step.shape[1]
    by_row = lambda w: pl.BlockSpec((QB, w), lambda i: (i, 0))
    fixed = lambda s: pl.BlockSpec(s, lambda i: (0, 0))
    return pl.pallas_call(
        scan_kernel,
        grid=(rows // QB,),
        in_specs=[by_row(width), by_row(N), by_row(N), by_row(heads),
                  pl.BlockSpec((heads, QB), lambda i: (0, i)), fixed((1, heads)), fixed((heads, 1))],
        out_specs=[by_row(width), by_row(heads), fixed((N, width)), fixed((1, width))],
        out_shape=[jax.ShapeDtypeStruct((rows, width), F32),
                   jax.ShapeDtypeStruct((rows, heads), F32),
                   jax.ShapeDtypeStruct((N, width), LOW),
                   jax.ShapeDtypeStruct((1, width), F32)],
        scratch_shapes=[pltpu.VMEM((N, width), F32), pltpu.VMEM((1, heads), F32)],
        cost_estimate=pl.CostEstimate(flops=rows * width * 2 * 4 * N, transcendentals=rows * QB * heads,
                                      bytes_accessed=rows * width * 8),
        name="local_scan",
    )(x, b, c, step, step.T, rate[None, :], rate[:, None])


def gate_kernel(whole_groups, y_ref, x_ref, c_ref, grown_ref, state_ref, z_ref, skip_ref, gain_ref, out_ref):
    heads = grown_ref.shape[1]
    grow = jnp.dot(jnp.exp(grown_ref[...]), head_spread(heads), precision=HIGH,
                   preferred_element_type=F32)
    carried = grow * jnp.dot(c_ref[...], state_ref[...], preferred_element_type=F32)
    full = y_ref[...] + carried + skip_ref[...] * x_ref[...].astype(F32)
    z = z_ref[...]
    gated = full * (z / (1.0 + jnp.exp(-z)))
    out_ref[...] = rms_norm(gated, gain_ref[...]).astype(LOW) if whole_groups else gated


def run_gate(y, x, c, grown, state, z, skip, gain, whole_groups):
    rows, width = y.shape
    heads = grown.shape[1]
    by_row = lambda w: pl.BlockSpec((QB, w), lambda i: (i, 0))
    fixed = lambda s: pl.BlockSpec(s, lambda i: (0, 0))
    return pl.pallas_call(
        functools.partial(gate_kernel, whole_groups),
        grid=(rows // QB,),
        in_specs=[by_row(width), by_row(width), by_row(N), by_row(heads), fixed((N, width)),
                  by_row(width), fixed((1, width)), fixed((1, width))],
        out_specs=by_row(width),
        out_shape=jax.ShapeDtypeStruct((rows, width), LOW if whole_groups else F32),
        cost_estimate=pl.CostEstimate(flops=rows * width * 2 * N, transcendentals=rows * width,
                                      bytes_accessed=rows * width * 12),
        name="gate_norm",
    )(y, x, c, grown, state, z, skip, gain)


def attend_kernel(where_ref, q_ref, k_ref, v_ref, out_ref, peak, mass, acc):
    rows = q_ref.shape[0]
    here = where_ref[0]
    reach = WINDOW // rows
    scale = HD ** (-0.5) * 1.4426950408889634
    q = q_ref[...]
    row = lax.broadcasted_iota(jnp.int32, (rows, rows), 0)
    col = lax.broadcasted_iota(jnp.int32, (rows, rows), 1)

    def scores_of(block):
        start = pl.multiple_of(block * rows, rows)
        return dot_nt(q, k_ref[pl.ds(start, rows), :]) * scale, v_ref[pl.ds(start, rows), :]

    def fold(scores, value):
        old = peak[...]
        new = jnp.maximum(old, jnp.max(scores, axis=1, keepdims=True))
        weights = jnp.exp2(scores - new)
        shrink = jnp.exp2(old - new)
        mass[...] = mass[...] * shrink + jnp.sum(weights, axis=1, keepdims=True)
        acc[...] = acc[...] * shrink + jnp.dot(weights.astype(LOW), value, preferred_element_type=F32)
        peak[...] = new

    scores, value = scores_of(here)
    scores = jnp.where(col <= row, scores, MASKED)
    first = jnp.max(scores, axis=1, keepdims=True)
    weights = jnp.exp2(scores - first)
    peak[...] = first
    mass[...] = jnp.sum(weights, axis=1, keepdims=True)
    acc[...] = jnp.dot(weights.astype(LOW), value, preferred_element_type=F32)

    def step(block, carry):
        fold(*scores_of(block))
        return carry

    lax.fori_loop(jnp.maximum(here - reach + 1, 0), here, step, 0)

    @pl.when(here >= reach)
    def _():
        far, far_value = scores_of(jnp.maximum(here - reach, 0))
        fold(jnp.where(col > row, far, MASKED), far_value)

    out_ref[...] = acc[...] / mass[...]


def run_attention(where, q, kv):
    rows, width = q.shape
    heads = width // HD
    kv_heads = kv.shape[1] // (2 * HD)
    per = heads // kv_heads
    keys = kv.shape[0]
    return pl.pallas_call(
        attend_kernel,
        grid_spec=pltpu.PrefetchScalarGridSpec(
            num_scalar_prefetch=1,
            grid=(heads,),
            in_specs=[pl.BlockSpec((rows, HD), lambda h, w: (0, h)),
                      pl.BlockSpec((keys, HD), lambda h, w: (0, h // per)),
                      pl.BlockSpec((keys, HD), lambda h, w: (0, kv_heads + h // per))],
            out_specs=pl.BlockSpec((rows, HD), lambda h, w: (0, h)),
            scratch_shapes=[pltpu.VMEM((rows, 1), F32), pltpu.VMEM((rows, 1), F32),
                            pltpu.VMEM((rows, HD), F32)],
        ),
        out_shape=jax.ShapeDtypeStruct((rows, width), F32),
        cost_estimate=pl.CostEstimate(flops=4 * rows * keys * width,
                                      transcendentals=rows * keys * heads,
                                      bytes_accessed=8 * rows * width),
        name="window_attend",
    )(where, q, kv, kv)


def on_device(
    hidden_in,
    norm_gain,
    w_z,
    w_x,
    w_b,
    w_c,
    w_dt,
    conv_x,
    conv_b,
    conv_c,
    dt_bias,
    a_rate,
    skip_gain,
    group_gain,
    w_out,
    attn_gain,
    w_q,
    w_k,
    w_v,
):
    rows_here = hidden_in.shape[0]
    place = lax.axis_index("seq")
    core = place % 2
    chip = place // 2

    def half(array, which, axis):
        width = array.shape[axis] // 2
        return lax.dynamic_slice_in_dim(array, which * width, width, axis)

    whole_groups = conv_b.shape[1] // N > 1

    def group_half(array, which):
        return half(array, which, 1) if whole_groups else array

    def half_columns(which):
        return jnp.concatenate(
            [half(w_x, which, 1), group_half(w_b, which), group_half(w_c, which), half(w_dt, which, 1)],
            axis=1,
        )

    def own_rows(mine, theirs, axis):
        return in_core_order(core, mine, swap_cores(theirs), axis)

    w_in = gather_chips(own_rows(half_columns(core), half_columns(1 - core), 0), 0)
    w_gate = gather_chips(own_rows(half(w_z, core, 1), half(w_z, 1 - core, 1), 0), 0)
    w_back = gather_chips(own_rows(half(w_out, core, 0), half(w_out, 1 - core, 0), 1), 1)

    whole_rows = gather_features(hidden_in)
    normed = rms_norm(whole_rows.astype(F32), norm_gain).astype(LOW)
    normed = in_core_order(core, normed, swap_cores(normed), 0)

    taps = jnp.concatenate(
        [half(conv_x, core, 1), group_half(conv_b, core), group_half(conv_c, core)], axis=1
    )
    mapped = jnp.dot(normed, w_in, preferred_element_type=F32)
    conv_width = taps.shape[1]
    x_width = conv_x.shape[1] // 2
    to_conv = mapped[:, :conv_width]
    rim_rows = taps.shape[0] - 1
    length = to_conv.shape[0]
    count = lax.axis_size("seq")
    rim = lax.ppermute(
        to_conv[length - rim_rows :], "seq", [(i, i + 2) for i in range(count - 2)]
    )
    padded = jnp.concatenate([rim, to_conv], axis=0)
    summed = jnp.zeros(to_conv.shape, F32)
    for offset in range(taps.shape[0]):
        summed = summed + taps[offset][None, :] * padded[offset : offset + length]
    conv = jax.nn.silu(summed).astype(LOW)
    x = conv[:, :x_width]
    b = conv[:, x_width : x_width + N]
    c = conv[:, x_width + N :]
    step = jax.nn.softplus(mapped[:, conv_width:] + half(dt_bias, core, 0)[None, :])
    y, grown, state, total = run_scan(x, b, c, step, half(a_rate, core, 0))

    states = gather_chips(state[None], 0)
    totals = gather_chips(total, 0)
    incoming = jnp.zeros(state.shape, F32)
    for turn in range(count // 2 - 1):
        passed = totals[turn][None, :] * incoming + states[turn].astype(F32)
        incoming = jnp.where(turn < chip, passed, incoming)

    gate_proj = jnp.dot(normed, w_gate, preferred_element_type=F32)
    skip = jnp.repeat(half(skip_gain, core, 0), P_SIZE)[None, :]
    gain = half(group_gain, core, 0)[None, :]
    y_normed = run_gate(y, x, c, grown, incoming.astype(LOW), gate_proj, skip, gain, whole_groups)
    if not whole_groups:
        squares = jnp.sum(y_normed * y_normed, axis=1, keepdims=True)
        mean = (squares + swap_cores(squares)) / (2 * x_width)
        y_normed = (y_normed * lax.rsqrt(mean + 1e-05) * gain).astype(LOW)
    theirs = jnp.dot(half(y_normed, 1 - core, 0), w_back, preferred_element_type=F32).astype(LOW)
    came = swap_cores(theirs)
    mine = jnp.dot(half(y_normed, core, 0), w_back, preferred_element_type=F32)
    part = (mine + came.astype(F32)).astype(LOW)
    mixed = hidden_in.astype(F32) + scatter_features(part)
    stream_rows = gather_features(mixed.astype(LOW))
    normed_two = rms_norm(stream_rows.astype(F32), attn_gain).astype(LOW)
    w_kv = jnp.concatenate([w_k, w_v], axis=1)
    own_kv = jnp.dot(normed_two, w_kv, preferred_element_type=F32).astype(LOW)
    kv = lax.all_gather(own_kv, "seq", axis=0, tiled=True)
    queries = jnp.dot(normed_two, w_q, preferred_element_type=F32).astype(LOW)
    context = run_attention(place.astype(jnp.int32)[None], queries, kv)
    return (mixed, context)


def solution(mesh):
    placed = (
        P("seq", "mp"),
        P(),
        P("seq", "mp"),
        P("seq", "mp"),
        P("seq", "mp"),
        P("seq", "mp"),
        P("seq", "mp"),
        P(None, "mp"),
        P(None, "mp"),
        P(None, "mp"),
        P("mp"),
        P("mp"),
        P("mp"),
        P("mp"),
        P("mp", "seq"),
        P(),
        P(None, "mp"),
        P(None, "mp"),
        P(None, "mp"),
    )
    return jax.shard_map(
        on_device,
        mesh=mesh,
        in_specs=placed,
        out_specs=(P("seq", "mp"), P("seq", "mp")),
        check_vma=False,
    )
```
